32 devices in a mesh: dp: 8 (over z, x), mp: 4 (over y, core).
Axes of the slice: x: 2, y: 2, z: 4, core: 2. Of those that a mesh axis runs over, the one named last changes fastest.
Arguments:
- features: bfloat16 [2048, 512], P('dp'), may hold values from -6 to 6
- adjacency: bfloat16 [64, 32, 128, 128], P('dp'), may hold values from -0.125 to 0.125
- source_block: int32 [64, 32], P('dp'), may hold values from 0 to 1
- edge_type: int32 [64, 32], P('dp'), may hold values from 0 to 19
- target_block: int32 [64, 32], P('dp'), may hold values from 0 to 1
- live_count: int32 [8, 8], P('dp'), may hold values from 24 to 32, as said below
- relation_weight: bfloat16 [20, 512, 512], P(None, None, 'mp'), may hold values from -0.25 to 0.25
- self_weight: bfloat16 [512, 512], P(None, 'mp'), may hold values from -0.25 to 0.25
- layer_bias: bfloat16 [512], P('mp'), may hold values from -3 to 3
- norm_gain: bfloat16 [512], replicated, may hold values from 0.5 to 1.5
Outputs:
- node_states: bfloat16 [2048, 512], P(('dp', 'mp'))
The draws below stay inside these ranges and needn't reach their ends.
Inputs may be any that keep to these rules, and one draw needn't show every extreme that they name: `source_block`: row s * 8 + d names a block among sender s's 2 blocks. `target_block`: row d * 8 + s names a block among receiver d's 2 blocks. live_count[d, s] live slots from sender s to receiver d, the first ones; some receiver has all 32 slots live from every sender.
All inputs are finite; a program needn't handle non-finite values.
Results may differ from the reference program's by a relative error of at most 0.007.
Values may be sent and summed in bfloat16 or wider, within the bound.
A program may use at most 128 MiB of HBM per device.

```python
import jax
import jax.numpy as jnp
from jax import lax

D = 512
R = 20
BLK = 128
NB_DEV = 2
IN_DEV = 256
PEERS = 8
SLOTS = 32
PAIRS = 64
NODES = 2048


def draw_live_count(key, part):
    lowest = max(1, 3 * SLOTS // 4)
    drawn = jax.random.randint(jax.random.fold_in(key, 11), (PEERS, PEERS), lowest, SLOTS + 1)
    full_row = jax.random.randint(jax.random.fold_in(key, 12), (), 0, PEERS)
    row_index = jnp.arange(PEERS)[:, None]
    return jnp.where(row_index == full_row, SLOTS, drawn).astype(jnp.int32)


def with_ends(values, rng, smallest, largest):
    longest = values.shape.index(max(values.shape))
    spots = []
    for shift in (0, 1):
        where = [jax.random.randint(jax.random.fold_in(rng, axis), (), 0, length) for axis, length in enumerate(values.shape)]
        where[longest] = (where[longest] + shift) % values.shape[longest]
        spots.append(tuple(where))
    return values.at[spots[0]].set(smallest).at[spots[1]].set(largest)


def level_of(key, shape, shards, smallest, largest):
    def one(position, parts):
        draws = jax.random.uniform(jax.random.fold_in(jax.random.fold_in(key, 6), position), (parts,), jnp.float32, smallest / len(shards), largest / len(shards))
        return jnp.repeat(jnp.exp(draws), shape[position] // parts).reshape((-1,) + (1,) * (len(shape) - position - 1))

    factor_of = one(*shards[0])
    for cut in shards[1:]:
        factor_of = factor_of * one(*cut)
    return factor_of


def noise(rng, dims, deviation, limit, cuts=(), held_as=jnp.bfloat16):
    values = jax.random.normal(rng, dims, jnp.float32) * deviation
    if len(cuts) > 0:
        values = level_of(rng, dims, cuts, -0.22, 0.18) * values
    return jnp.clip(values, min=-limit, max=limit).astype(held_as)


def setup_inputs(seed: int = 0) -> dict:
    streams_of = jax.random.split(jax.random.key(seed), 11)
    features = noise(streams_of[0], (NODES, D), 1.0, 6.0, ((0, 8),))
    adjacency = noise(streams_of[1], (PAIRS, SLOTS, BLK, BLK), ((BLK * IN_DEV // NB_DEV) ** -0.5), 0.125, ((0, 8),))
    source_block = with_ends(jax.random.randint(streams_of[2], (PAIRS, SLOTS), 0, NB_DEV), jax.random.fold_in(streams_of[2], 1), 0, NB_DEV - 1).astype(jnp.int32)
    edge_type = with_ends(jax.random.randint(streams_of[3], (PAIRS, SLOTS), 0, R), jax.random.fold_in(streams_of[3], 1), 0, R - 1).astype(jnp.int32)
    target_block = with_ends(jax.random.randint(streams_of[4], (PAIRS, SLOTS), 0, NB_DEV), jax.random.fold_in(streams_of[4], 1), 0, NB_DEV - 1).astype(jnp.int32)
    live_count = draw_live_count(jax.random.fold_in(streams_of[10], 71), 0)
    relation_weight = noise(streams_of[6], (R, D, D), D ** -0.5, 0.25, ((2, 4),))
    self_weight = noise(streams_of[7], (D, D), D ** -0.5, 0.25, ((1, 4),))
    layer_bias = noise(streams_of[8], (D,), 0.5, 3.0, ((0, 4),))
    norm_gain = jnp.clip(1.0 + 0.1 * jax.random.normal(streams_of[9], (D,), jnp.float32), 0.5, 1.5).astype(jnp.bfloat16)
    return dict(features=features, adjacency=adjacency, source_block=source_block, edge_type=edge_type, target_block=target_block, live_count=live_count, relation_weight=relation_weight, self_weight=self_weight, layer_bias=layer_bias, norm_gain=norm_gain)


epsilon = 1e-05

def reference(features, adjacency, source_block, edge_type, target_block, live_count, relation_weight, self_weight, layer_bias, norm_gain):
    stacked = features.reshape(PEERS, NB_DEV, BLK, D)
    adj_tiles = adjacency.reshape(PEERS, PEERS * SLOTS, BLK, BLK)
    lookup_rows = (source_block * R + edge_type).reshape(PEERS, PEERS * SLOTS).astype(jnp.int32)
    active = jnp.arange(SLOTS, dtype=jnp.int32)[None, None, :] < live_count[:, :, None]
    matches = target_block.reshape(PEERS, PEERS, SLOTS)[:, :, :, None] == jnp.arange(NB_DEV, dtype=jnp.int32)[None, None, None, :]
    selector = jnp.logical_and(matches, active[:, :, :, None]).astype(jnp.float32)
    per_sender = jnp.transpose(selector, (1, 0, 2, 3))
    relations = relation_weight.astype(jnp.float32)

    def one_sender(running, inputs):
        block_rows, sender_tiles, sender_rows, sender_select = inputs
        lookup = jnp.einsum('bid,rdc->bric', block_rows.astype(jnp.float32), relations).astype(jnp.bfloat16)
        lookup = lookup.reshape(NB_DEV * R, BLK, D)
        chosen = jnp.take(lookup, sender_rows, axis=0)
        message = jnp.einsum('nij,njc->nic', sender_tiles.astype(jnp.float32), chosen.astype(jnp.float32))
        message = message.reshape(PEERS, SLOTS, BLK * D)
        summed = jnp.einsum('rkb,rkx->rbx', sender_select, message, precision=lax.Precision.HIGHEST)
        return (running + summed, None)
    initial = jnp.zeros((PEERS, NB_DEV, BLK * D), jnp.float32)
    running, ignored = lax.scan(one_sender, initial, (stacked, adj_tiles, lookup_rows, per_sender))
    aggregate = running.reshape(PEERS * NB_DEV * BLK, D)
    own_term = jnp.dot(features, self_weight, preferred_element_type=jnp.float32)
    hidden = jax.nn.relu(own_term + aggregate + layer_bias.astype(jnp.float32)).astype(jnp.bfloat16)
    values = lax.optimization_barrier(hidden).astype(jnp.float32)
    inverse_rms = lax.rsqrt(lax.optimization_barrier(jnp.mean(values * values, axis=1, keepdims=True)) + epsilon)
    return (values * inverse_rms * norm_gain.astype(jnp.float32)).astype(jnp.bfloat16)
```

```python
import functools

import jax
import jax.numpy as jnp
from jax import lax
from jax.experimental import pallas as pl
from jax.experimental.pallas import tpu as pltpu
from jax.sharding import PartitionSpec as P

BLK = 128
PAIR = 2
LANES = 128
epsilon = 1e-05


def kernel(
    peers,
    groups,
    x_ref,
    sb_ref,
    et_ref,
    tb_ref,
    lc_ref,
    sw_ref,
    bias_ref,
    gain_ref,
    adj_hbm,
    rw_hbm,
    out_ref,
    adj,
    rw,
    table,
    code_out,
    code_in,
    code_sm,
    own,
    pbuf,
    rbuf,
    zbuf,
    zin,
    hid,
    gath,
    rw_sem,
    adj_sem,
    code_send,
    code_recv,
    sm_sem,
    x_send,
    x_recv,
    z_send,
    z_recv,
    h_send,
    h_recv,
):
    me = lax.axis_index("dp")
    col = lax.axis_index("mp")
    outer = peers // PAIR
    zz = me // PAIR
    xx = me % PAIR
    relations = rw_hbm.shape[0]
    slots = adj_hbm.shape[1]
    rows = x_ref.shape[0]
    blocks = rows // BLK
    columns = sw_ref.shape[1]
    zero_tile = blocks * relations
    part = rows // groups

    def dp_peer(offset):
        return lax.rem(me + offset, peers)

    def mp_peer(offset):
        return lax.rem(col + offset, groups)

    barrier = pltpu.get_barrier_semaphore()
    for offset in range(1, peers):
        pl.semaphore_signal(barrier, inc=1, device_id={"dp": dp_peer(offset)})
    for offset in range(1, groups):
        pl.semaphore_signal(barrier, inc=1, device_id={"mp": mp_peer(offset)})

    rw_copies = [
        pltpu.make_async_copy(rw_hbm.at[pl.ds(r, 2)], rw.at[pl.ds(r, 2)], rw_sem.at[r // 2])
        for r in range(0, relations, 2)
    ]
    for copy in rw_copies:
        copy.start()

    def receiver_of(i, side):
        return lax.rem(zz + 1 + i, outer) * PAIR + side

    def adj_copy(d):
        return pltpu.make_async_copy(adj_hbm.at[d], adj.at[d], adj_sem.at[d])

    def start_adj(side):
        def go(i, carry):
            adj_copy(receiver_of(i, side)).start()
            return carry

        lax.fori_loop(0, outer, go, 0)

    start_adj(1 - xx)
    start_adj(xx)

    code_out[...] = jnp.full(code_out.shape, -1, jnp.int32)
    slot_ids = lax.broadcasted_iota(jnp.int32, (1, slots), 1)
    for s in range(peers):
        live = slot_ids < lc_ref[0, s]
        code_out[s, :, 0:slots] = jnp.where(live, tb_ref[s : s + 1, :], -1)
    table[zero_tile] = jnp.zeros((BLK, columns), jnp.bfloat16)

    pl.semaphore_wait(barrier, peers - 1 + groups - 1)

    def code_copy(offset):
        to = dp_peer(offset)
        return pltpu.make_async_remote_copy(
            src_ref=code_out.at[to],
            dst_ref=code_in.at[me],
            send_sem=code_send.at[offset],
            recv_sem=code_recv.at[offset],
            device_id={"dp": to},
        )

    for offset in range(1, peers):
        code_copy(offset).start()
    code_in[me] = code_out[me]

    x = x_ref[...]
    for r in range(0, relations, 2):
        rw_copies[r // 2].wait()
        w = jnp.concatenate([rw[r], rw[r + 1]], axis=1)
        t = jnp.dot(x, w, preferred_element_type=jnp.float32).astype(jnp.bfloat16)
        for b in range(blocks):
            for j in range(2):
                table[b * relations + r + j] = t[
                    b * BLK : (b + 1) * BLK, j * columns : (j + 1) * columns
                ]
    base = jnp.dot(x, sw_ref[...], preferred_element_type=jnp.float32)
    own[...] = base + bias_ref[...].astype(jnp.float32)

    for offset in range(1, peers):
        code_copy(offset).wait()
    to_smem = pltpu.make_async_copy(code_in, code_sm, sm_sem)
    to_smem.start()
    to_smem.wait()

    def sums(d):
        adj_copy(d).wait()
        acc = jnp.zeros((BLK, blocks * columns), jnp.float32)
        step = 2
        for k in range(0, slots, step):
            lhs, rhs = [], []
            for j in range(k, k + step):
                code = code_sm[d, 0, j]
                row = sb_ref[d, j] * relations + et_ref[d, j]
                lhs.append(adj[d, j])
                rhs.append(
                    jnp.concatenate(
                        [table[jnp.where(code == b, row, zero_tile)] for b in range(blocks)],
                        axis=1,
                    )
                )
            acc = acc + jnp.dot(
                jnp.concatenate(lhs, axis=1),
                jnp.concatenate(rhs, axis=0),
                preferred_element_type=jnp.float32,
            )
        return jnp.concatenate(
            [acc[:, b * columns : (b + 1) * columns] for b in range(blocks)], axis=0
        )

    def x_copy(i):
        return pltpu.make_async_remote_copy(
            src_ref=pbuf.at[i],
            dst_ref=rbuf.at[i],
            send_sem=x_send.at[i],
            recv_sem=x_recv.at[i],
            device_id={"dp": zz * PAIR + 1 - xx},
        )

    def z_copy(i):
        return pltpu.make_async_remote_copy(
            src_ref=zbuf.at[i],
            dst_ref=zin.at[i],
            send_sem=z_send.at[i],
            recv_sem=z_recv.at[i],
            device_id={"dp": receiver_of(i, xx)},
        )

    def partner_step(i, carry):
        pbuf[i] = sums(receiver_of(i, 1 - xx)).astype(jnp.bfloat16)
        x_copy(i).start()
        return carry

    lax.fori_loop(0, outer, partner_step, 0)

    def own_step(i, carry):
        mine = sums(receiver_of(i, xx))
        x_copy(i).wait()
        zbuf[i] = (mine + rbuf[i].astype(jnp.float32)).astype(jnp.bfloat16)
        z_copy(i).start()
        return carry

    lax.fori_loop(0, outer - 1, own_step, 0)

    own[...] += sums(me)
    x_copy(outer - 1).wait()
    own[...] += rbuf[outer - 1].astype(jnp.float32)

    def arrive(i, carry):
        z_copy(i).wait()
        own[...] += zin[i].astype(jnp.float32)
        return carry

    lax.fori_loop(0, outer - 1, arrive, 0)

    hid[...] = jnp.maximum(own[...], 0.0).astype(jnp.bfloat16)

    def h_copy(offset):
        to = mp_peer(offset)
        return pltpu.make_async_remote_copy(
            src_ref=hid.at[pl.ds(pl.multiple_of(to * part, part), part)],
            dst_ref=gath.at[col],
            send_sem=h_send.at[offset],
            recv_sem=h_recv.at[offset],
            device_id={"mp": to},
        )

    for offset in range(1, groups):
        h_copy(offset).start()
    gath[col] = hid[pl.ds(pl.multiple_of(col * part, part), part)]
    for offset in range(1, groups):
        h_copy(offset).wait()
    values = jnp.concatenate([gath[g] for g in range(groups)], axis=1).astype(jnp.float32)
    inverse_rms = lax.rsqrt(jnp.mean(values * values, axis=1, keepdims=True) + epsilon)
    out_ref[...] = (values * inverse_rms * gain_ref[...].astype(jnp.float32)).astype(jnp.bfloat16)


def per_device(
    features,
    adjacency,
    source_block,
    edge_type,
    target_block,
    live_count,
    relation_weight,
    self_weight,
    layer_bias,
    norm_gain,
):
    peers = lax.axis_size("dp")
    groups = lax.axis_size("mp")
    rows, width = features.shape
    relations, _, columns = relation_weight.shape
    blocks = rows // BLK
    outer = peers // PAIR
    part = rows // groups
    vmem = pl.BlockSpec(memory_space=pltpu.VMEM)
    smem = pl.BlockSpec(memory_space=pltpu.SMEM)
    hbm = pl.BlockSpec(memory_space=pl.ANY)
    dma = pltpu.SemaphoreType.DMA
    return pl.pallas_call(
        functools.partial(kernel, peers, groups),
        out_shape=jax.ShapeDtypeStruct((part, width), jnp.bfloat16),
        in_specs=[vmem, smem, smem, vmem, smem, vmem, vmem, vmem, hbm, hbm],
        out_specs=vmem,
        scratch_shapes=[
            pltpu.VMEM(adjacency.shape, jnp.bfloat16),
            pltpu.VMEM(relation_weight.shape, jnp.bfloat16),
            pltpu.VMEM((blocks * relations + 1, BLK, columns), jnp.bfloat16),
            pltpu.VMEM((peers, 1, LANES), jnp.int32),
            pltpu.VMEM((peers, 1, LANES), jnp.int32),
            pltpu.SMEM((peers, 1, LANES), jnp.int32),
            pltpu.VMEM((rows, columns), jnp.float32),
            pltpu.VMEM((outer, rows, columns), jnp.bfloat16),
            pltpu.VMEM((outer, rows, columns), jnp.bfloat16),
            pltpu.VMEM((outer, rows, columns), jnp.bfloat16),
            pltpu.VMEM((outer, rows, columns), jnp.bfloat16),
            pltpu.VMEM((rows, columns), jnp.bfloat16),
            pltpu.VMEM((groups, part, columns), jnp.bfloat16),
            dma((relations // 2,)),
            dma((peers,)),
            dma((peers,)),
            dma((peers,)),
            dma,
            dma((outer,)),
            dma((outer,)),
            dma((outer,)),
            dma((outer,)),
            dma((groups,)),
            dma((groups,)),
        ],
        compiler_params=pltpu.CompilerParams(collective_id=0, has_side_effects=True),
    )(
        features,
        source_block,
        edge_type,
        target_block,
        live_count,
        self_weight,
        layer_bias.reshape(1, columns),
        norm_gain.reshape(1, width),
        adjacency,
        relation_weight,
    )


def solution(mesh):
    return jax.shard_map(
        per_device,
        mesh=mesh,
        in_specs=(
            P("dp", None),
            P("dp", None, None, None),
            P("dp", None),
            P("dp", None),
            P("dp", None),
            P("dp", None),
            P(None, None, "mp"),
            P(None, "mp"),
            P("mp"),
            P(),
        ),
        out_specs=P(("dp", "mp"), None),
        check_vma=False,
    )
```

```python
import functools

import jax
import jax.numpy as jnp
from jax import lax
from jax.experimental import pallas as pl
from jax.experimental.pallas import tpu as pltpu
from jax.sharding import PartitionSpec as P

BLK = 128
PAIR = 2
LANES = 128
epsilon = 1e-05


def kernel(
    peers,
    groups,
    x_hbm,
    sb_hbm,
    et_hbm,
    tb_hbm,
    lc_hbm,
    sw_hbm,
    bias_hbm,
    gain_hbm,
    adj_hbm,
    rw_hbm,
    out_ref,
    x_ref,
    sb_ref,
    et_ref,
    tb_ref,
    lc_ref,
    sw_ref,
    bias_ref,
    gain_ref,
    adj,
    rw,
    table,
    code_out,
    code_in,
    code_sm,
    own,
    pbuf,
    rbuf,
    zbuf,
    zin,
    in_sem,
    rw_sem,
    adj_sem,
    code_send,
    code_recv,
    sm_sem,
    x_send,
    x_recv,
    z_send,
    z_recv,
):
    me = lax.axis_index("dp")
    col = lax.axis_index("mp")
    outer = peers // PAIR
    zz = me // PAIR
    xx = me % PAIR
    relations = rw_hbm.shape[0]
    slots = adj_hbm.shape[1]
    rows = x_hbm.shape[0]
    blocks = rows // BLK
    columns = sw_hbm.shape[1]
    zero_tile = blocks * relations
    part = rows // groups

    def dp_peer(offset):
        return lax.rem(me + offset, peers)

    def mp_peer(offset):
        return lax.rem(col + offset, groups)

    def z_peer(offset):
        return lax.rem(zz + offset, outer)

    barrier = pltpu.get_barrier_semaphore()
    for zo in range(outer):
        pl.semaphore_signal(barrier, inc=1, device_id={"dp": z_peer(zo) * PAIR + 1 - xx})
        for mo in range(groups):
            if zo or mo:
                pl.semaphore_signal(
                    barrier, inc=1, device_id={"dp": z_peer(zo) * PAIR + xx, "mp": mp_peer(mo)}
                )

    pairs = (
        (tb_hbm, tb_ref),
        (lc_hbm, lc_ref),
        (x_hbm, x_ref),
        (sb_hbm, sb_ref),
        (et_hbm, et_ref),
        (sw_hbm, sw_ref),
        (bias_hbm, bias_ref),
        (gain_hbm, gain_ref),
    )
    in_copies = [
        pltpu.make_async_copy(src, dst, in_sem.at[n]) for n, (src, dst) in enumerate(pairs)
    ]
    for copy in in_copies[:3]:
        copy.start()

    rw_copies = [
        pltpu.make_async_copy(rw_hbm.at[pl.ds(r, 2)], rw.at[pl.ds(r, 2)], rw_sem.at[r // 2])
        for r in range(0, relations, 2)
    ]
    for copy in rw_copies:
        copy.start()
    for copy in in_copies[3:]:
        copy.start()

    def receiver_of(i, side):
        down = outer - 1 - i
        down = jnp.where(down <= zz, down - 1, down)
        up = jnp.where(i < zz, i, i + 1)
        to = jnp.where(zz < outer // 2, down, up)
        return jnp.where(i == outer - 1, zz, to) * PAIR + side

    def adj_copy(d):
        return pltpu.make_async_copy(adj_hbm.at[d], adj.at[d], adj_sem.at[d])

    def start_adj(side):
        def go(i, carry):
            adj_copy(receiver_of(i, side)).start()
            return carry

        lax.fori_loop(0, outer, go, 0)

    start_adj(1 - xx)
    start_adj(xx)

    in_copies[0].wait()
    in_copies[1].wait()
    code_out[...] = jnp.full(code_out.shape, -1, jnp.int32)
    slot_ids = lax.broadcasted_iota(jnp.int32, (1, slots), 1)
    for s in range(peers):
        live = slot_ids < lc_ref[0, s]
        code_out[s, :, 0:slots] = jnp.where(live, tb_ref[s : s + 1, :], -1)
    table[zero_tile] = jnp.zeros((BLK, columns), jnp.bfloat16)

    in_copies[2].wait()
    x = x_ref[...]
    for r in range(0, relations, 2):
        rw_copies[r // 2].wait()
        w = jnp.concatenate([rw[r], rw[r + 1]], axis=1)
        t = jnp.dot(x, w, preferred_element_type=jnp.float32).astype(jnp.bfloat16)
        for b in range(blocks):
            for j in range(2):
                table[b * relations + r + j] = t[
                    b * BLK : (b + 1) * BLK, j * columns : (j + 1) * columns
                ]

    pl.semaphore_wait(barrier, outer * groups - 1 + outer)

    def code_copy(offset):
        to = dp_peer(offset)
        return pltpu.make_async_remote_copy(
            src_ref=code_out.at[to],
            dst_ref=code_in.at[me],
            send_sem=code_send.at[offset],
            recv_sem=code_recv.at[offset],
            device_id={"dp": to},
        )

    for offset in range(1, peers):
        code_copy(offset).start()
    code_in[me] = code_out[me]

    for copy in in_copies[3:]:
        copy.wait()
    base = jnp.dot(x, sw_ref[...], preferred_element_type=jnp.float32)
    own[...] = base + bias_ref[...].astype(jnp.float32)

    for offset in range(1, peers):
        code_copy(offset).wait()
    to_smem = pltpu.make_async_copy(code_in, code_sm, sm_sem)
    to_smem.start()
    to_smem.wait()

    def sums(d):
        adj_copy(d).wait()
        acc = jnp.zeros((BLK, blocks * columns), jnp.float32)
        step = 2
        for k in range(0, slots, step):
            lhs, rhs = [], []
            for j in range(k, k + step):
                code = code_sm[d, 0, j]
                row = sb_ref[d, j] * relations + et_ref[d, j]
                lhs.append(adj[d, j])
                rhs.append(
                    jnp.concatenate(
                        [table[jnp.where(code == b, row, zero_tile)] for b in range(blocks)],
                        axis=1,
                    )
                )
            acc = acc + jnp.dot(
                jnp.concatenate(lhs, axis=1),
                jnp.concatenate(rhs, axis=0),
                preferred_element_type=jnp.float32,
            )
        return jnp.concatenate(
            [acc[:, b * columns : (b + 1) * columns] for b in range(blocks)], axis=0
        )

    def x_copy(i):
        return pltpu.make_async_remote_copy(
            src_ref=pbuf.at[i],
            dst_ref=rbuf.at[i],
            send_sem=x_send.at[i],
            recv_sem=x_recv.at[i],
            device_id={"dp": zz * PAIR + 1 - xx},
        )

    def z_copy(i, to, group, src):
        return pltpu.make_async_remote_copy(
            src_ref=zbuf.at[i, pl.ds(pl.multiple_of(group * part, part), part)],
            dst_ref=zin.at[src],
            send_sem=z_send.at[i, group],
            recv_sem=z_recv.at[src],
            device_id={"dp": to, "mp": group},
        )

    mine = zz * groups + col

    def partner_step(i, carry):
        pbuf[i] = sums(receiver_of(i, 1 - xx)).astype(jnp.bfloat16)
        x_copy(i).start()
        return carry

    lax.fori_loop(0, outer, partner_step, 0)

    def own_step(i, carry):
        held = sums(receiver_of(i, xx))
        x_copy(i).wait_recv()
        zbuf[i] = (held + rbuf[i].astype(jnp.float32)).astype(jnp.bfloat16)
        for mo in range(groups):
            z_copy(i, receiver_of(i, xx), mp_peer(mo), mine).start()
        return carry

    lax.fori_loop(0, outer - 1, own_step, 0)

    last = outer - 1
    held = own[...] + sums(me)
    x_copy(last).wait_recv()
    zbuf[last] = (held + rbuf[last].astype(jnp.float32)).astype(jnp.bfloat16)
    for mo in range(1, groups):
        z_copy(last, me, mp_peer(mo), mine).start()
    zin[mine] = zbuf[last, pl.ds(pl.multiple_of(col * part, part), part)]

    for i in range(outer):
        x_copy(i).wait_send()
        for mo in range(0 if i < last else 1, groups):
            z_copy(i, receiver_of(i, xx), mp_peer(mo), mine).wait_send()
    total = outer * groups
    for n in range(1, total):
        z_copy(0, me, mp_peer(1), lax.rem(mine + n, total)).wait_recv()
    pieces = []
    for g in range(groups):
        piece = zin[g].astype(jnp.float32)
        for z in range(1, outer):
            piece = piece + zin[z * groups + g].astype(jnp.float32)
        pieces.append(jnp.maximum(piece, 0.0).astype(jnp.bfloat16).astype(jnp.float32))
    values = jnp.concatenate(pieces, axis=1)
    gain = jnp.concatenate([gain_ref[n : n + 1, :] for n in range(gain_ref.shape[0])], axis=1)
    inverse_rms = lax.rsqrt(jnp.mean(values * values, axis=1, keepdims=True) + epsilon)
    out_ref[...] = (values * inverse_rms * gain.astype(jnp.float32)).astype(jnp.bfloat16)


def per_device(
    features,
    adjacency,
    source_block,
    edge_type,
    target_block,
    live_count,
    relation_weight,
    self_weight,
    layer_bias,
    norm_gain,
):
    peers = lax.axis_size("dp")
    groups = lax.axis_size("mp")
    rows, width = features.shape
    relations, _, columns = relation_weight.shape
    blocks = rows // BLK
    outer = peers // PAIR
    part = rows // groups
    vmem = pl.BlockSpec(memory_space=pltpu.VMEM)
    hbm = pl.BlockSpec(memory_space=pl.ANY)
    dma = pltpu.SemaphoreType.DMA
    return pl.pallas_call(
        functools.partial(kernel, peers, groups),
        out_shape=jax.ShapeDtypeStruct((part, width), jnp.bfloat16),
        in_specs=[hbm] * 10,
        out_specs=vmem,
        scratch_shapes=[
            pltpu.VMEM(features.shape, jnp.bfloat16),
            pltpu.SMEM(source_block.shape, jnp.int32),
            pltpu.SMEM(edge_type.shape, jnp.int32),
            pltpu.VMEM(target_block.shape, jnp.int32),
            pltpu.SMEM(live_count.shape, jnp.int32),
            pltpu.VMEM(self_weight.shape, jnp.bfloat16),
            pltpu.VMEM((1, columns), jnp.bfloat16),
            pltpu.VMEM((width // LANES, LANES), jnp.bfloat16),
            pltpu.VMEM(adjacency.shape, jnp.bfloat16),
            pltpu.VMEM(relation_weight.shape, jnp.bfloat16),
            pltpu.VMEM((blocks * relations + 1, BLK, columns), jnp.bfloat16),
            pltpu.VMEM((peers, 1, LANES), jnp.int32),
            pltpu.VMEM((peers, 1, LANES), jnp.int32),
            pltpu.SMEM((peers, 1, LANES), jnp.int32),
            pltpu.VMEM((rows, columns), jnp.float32),
            pltpu.VMEM((outer, rows, columns), jnp.bfloat16),
            pltpu.VMEM((outer, rows, columns), jnp.bfloat16),
            pltpu.VMEM((outer, rows, columns), jnp.bfloat16),
            pltpu.VMEM((outer * groups, part, columns), jnp.bfloat16),
            dma((8,)),
            dma((relations // 2,)),
            dma((peers,)),
            dma((peers,)),
            dma((peers,)),
            dma,
            dma((outer,)),
            dma((outer,)),
            dma((outer, groups)),
            dma((outer * groups,)),
        ],
        compiler_params=pltpu.CompilerParams(collective_id=0, has_side_effects=True),
    )(
        features,
        source_block,
        edge_type,
        target_block,
        live_count,
        self_weight,
        layer_bias.reshape(1, columns),
        norm_gain.reshape(width // LANES, LANES),
        adjacency,
        relation_weight,
    )


def solution(mesh):
    return jax.shard_map(
        per_device,
        mesh=mesh,
        in_specs=(
            P("dp", None),
            P("dp", None, None, None),
            P("dp", None),
            P("dp", None),
            P("dp", None),
            P("dp", None),
            P(None, None, "mp"),
            P(None, "mp"),
            P("mp"),
            P(),
        ),
        out_specs=P(("dp", "mp"), None),
        check_vma=False,
    )
```

```python
import functools

import jax
import jax.numpy as jnp
from jax import lax
from jax.experimental import pallas as pl
from jax.experimental.pallas import tpu as pltpu
from jax.sharding import PartitionSpec as P

BLK = 128
PAIR = 2
LANES = 128
epsilon = 1e-05


def kernel(
    peers,
    groups,
    x_hbm,
    sb_hbm,
    et_hbm,
    tb_hbm,
    lc_hbm,
    sw_hbm,
    bias_hbm,
    gain_hbm,
    adj_hbm,
    rw_hbm,
    out_ref,
    x_ref,
    sb_ref,
    et_ref,
    tb_ref,
    lc_ref,
    sw_ref,
    bias_ref,
    gain_ref,
    adj,
    rw,
    table,
    code_out,
    code_in,
    code_sm,
    own,
    pbuf,
    rbuf,
    zbuf,
    zin,
    in_sem,
    rw_sem,
    adj_sem,
    code_send,
    code_recv,
    sm_sem,
    x_send,
    x_recv,
    z_send,
    z_recv,
):
    me = lax.axis_index("dp")
    col = lax.axis_index("mp")
    outer = peers // PAIR
    zz = me // PAIR
    xx = me % PAIR
    relations = rw_hbm.shape[0]
    slots = adj_hbm.shape[1]
    rows = x_hbm.shape[0]
    blocks = rows // BLK
    columns = sw_hbm.shape[1]
    zero_tile = blocks * relations
    part = rows // groups

    def dp_peer(offset):
        return lax.rem(me + offset, peers)

    def mp_peer(offset):
        return lax.rem(col + offset, groups)

    def z_peer(offset):
        return lax.rem(zz + offset, outer)

    barrier = pltpu.get_barrier_semaphore()
    for zo in range(outer):
        pl.semaphore_signal(barrier, inc=1, device_id={"dp": z_peer(zo) * PAIR + 1 - xx})
        for mo in range(groups):
            if zo or mo:
                pl.semaphore_signal(
                    barrier, inc=1, device_id={"dp": z_peer(zo) * PAIR + xx, "mp": mp_peer(mo)}
                )

    pairs = (
        (tb_hbm, tb_ref),
        (lc_hbm, lc_ref),
        (x_hbm, x_ref),
        (sb_hbm, sb_ref),
        (et_hbm, et_ref),
        (sw_hbm, sw_ref),
        (bias_hbm, bias_ref),
        (gain_hbm, gain_ref),
    )
    in_copies = [
        pltpu.make_async_copy(src, dst, in_sem.at[n]) for n, (src, dst) in enumerate(pairs)
    ]
    for copy in in_copies[:3]:
        copy.start()

    rw_copies = [
        pltpu.make_async_copy(rw_hbm.at[pl.ds(r, 2)], rw.at[pl.ds(r, 2)], rw_sem.at[r // 2])
        for r in range(0, relations, 2)
    ]
    for copy in rw_copies:
        copy.start()
    for copy in in_copies[3:]:
        copy.start()

    def near_first(step):
        i = outer - 1 - step
        down = outer - 1 - i
        down = jnp.where(down <= zz, down - 1, down)
        up = jnp.where(i < zz, i, i + 1)
        to = jnp.where(zz < outer // 2, down, up)
        return jnp.where(i == outer - 1, zz, to)

    def adj_copy(d):
        return pltpu.make_async_copy(adj_hbm.at[d], adj.at[d], adj_sem.at[d])

    def start_adj(side):
        def go(i, carry):
            adj_copy(near_first(i) * PAIR + side).start()
            return carry

        lax.fori_loop(0, outer, go, 0)

    start_adj(1 - xx)
    start_adj(xx)

    in_copies[0].wait()
    in_copies[1].wait()
    code_out[...] = jnp.full(code_out.shape, -1, jnp.int32)
    slot_ids = lax.broadcasted_iota(jnp.int32, (1, slots), 1)
    for s in range(peers):
        live = slot_ids < lc_ref[0, s]
        code_out[s, :, 0:slots] = jnp.where(live, tb_ref[s : s + 1, :], -1)
    table[zero_tile] = jnp.zeros((BLK, columns), jnp.bfloat16)

    in_copies[2].wait()
    x = x_ref[...]
    for r in range(0, relations, 2):
        rw_copies[r // 2].wait()
        w = jnp.concatenate([rw[r], rw[r + 1]], axis=1)
        t = jnp.dot(x, w, preferred_element_type=jnp.float32).astype(jnp.bfloat16)
        for b in range(blocks):
            for j in range(2):
                table[b * relations + r + j] = t[
                    b * BLK : (b + 1) * BLK, j * columns : (j + 1) * columns
                ]

    pl.semaphore_wait(barrier, outer * groups - 1 + outer)

    def code_copy(offset):
        to = dp_peer(offset)
        return pltpu.make_async_remote_copy(
            src_ref=code_out.at[to],
            dst_ref=code_in.at[me],
            send_sem=code_send.at[offset],
            recv_sem=code_recv.at[offset],
            device_id={"dp": to},
        )

    for offset in range(1, peers):
        code_copy(offset).start()
    code_in[me] = code_out[me]

    for copy in in_copies[3:]:
        copy.wait()
    base = jnp.dot(x, sw_ref[...], preferred_element_type=jnp.float32)
    own[...] = base + bias_ref[...].astype(jnp.float32)

    def await_code(d):
        offset = lax.rem(me - d + peers, peers)
        pltpu.make_async_remote_copy(
            src_ref=code_out.at[d],
            dst_ref=code_in.at[d],
            send_sem=code_send.at[offset],
            recv_sem=code_recv.at[offset],
            device_id={"dp": d},
        ).wait_recv()

    def sums(d):
        to_smem = pltpu.make_async_copy(code_in.at[d], code_sm.at[d], sm_sem)
        to_smem.start()
        to_smem.wait()
        adj_copy(d).wait()
        acc = jnp.zeros((BLK, blocks * columns), jnp.float32)
        step = 2
        for k in range(0, slots, step):
            lhs, rhs = [], []
            for j in range(k, k + step):
                code = code_sm[d, 0, j]
                row = sb_ref[d, j] * relations + et_ref[d, j]
                lhs.append(adj[d, j])
                rhs.append(
                    jnp.concatenate(
                        [table[jnp.where(code == b, row, zero_tile)] for b in range(blocks)],
                        axis=1,
                    )
                )
            acc = acc + jnp.dot(
                jnp.concatenate(lhs, axis=1),
                jnp.concatenate(rhs, axis=0),
                preferred_element_type=jnp.float32,
            )
        return jnp.concatenate(
            [acc[:, b * columns : (b + 1) * columns] for b in range(blocks)], axis=0
        )

    def x_copy(i):
        return pltpu.make_async_remote_copy(
            src_ref=pbuf.at[i],
            dst_ref=rbuf.at[i],
            send_sem=x_send.at[i],
            recv_sem=x_recv.at[i],
            device_id={"dp": zz * PAIR + 1 - xx},
        )

    def z_copy(i, to, group, src):
        return pltpu.make_async_remote_copy(
            src_ref=zbuf.at[i, pl.ds(pl.multiple_of(group * part, part), part)],
            dst_ref=zin.at[src],
            send_sem=z_send.at[i, group],
            recv_sem=z_recv.at[src],
            device_id={"dp": to, "mp": group},
        )

    mine = zz * groups + col

    def partner_step(step, carry):
        z = near_first(step)
        d = z * PAIR + 1 - xx
        await_code(d)
        pbuf[z] = sums(d).astype(jnp.bfloat16)
        x_copy(z).start()
        return carry

    lax.fori_loop(0, outer, partner_step, 0)

    def own_step(step, carry):
        z = near_first(step)
        d = z * PAIR + xx
        await_code(d)
        held = sums(d)
        x_copy(z).wait_recv()
        zbuf[z] = (held + rbuf[z].astype(jnp.float32)).astype(jnp.bfloat16)
        for mo in range(groups):
            z_copy(z, d, mp_peer(mo), mine).start()
        return carry

    lax.fori_loop(1, outer, own_step, 0)

    held = own[...] + sums(me)
    x_copy(zz).wait_recv()
    zbuf[zz] = (held + rbuf[zz].astype(jnp.float32)).astype(jnp.bfloat16)
    for mo in range(1, groups):
        z_copy(zz, me, mp_peer(mo), mine).start()
    zin[mine] = zbuf[zz, pl.ds(pl.multiple_of(col * part, part), part)]

    for offset in range(1, peers):
        code_copy(offset).wait_send()
    for zo in range(outer):
        z = z_peer(zo)
        x_copy(z).wait_send()
        for mo in range(1 if zo == 0 else 0, groups):
            z_copy(z, z * PAIR + xx, mp_peer(mo), mine).wait_send()
    total = outer * groups
    for n in range(1, total):
        z_copy(0, me, mp_peer(1), lax.rem(mine + n, total)).wait_recv()
    pieces = []
    for g in range(groups):
        piece = zin[g].astype(jnp.float32)
        for z in range(1, outer):
            piece = piece + zin[z * groups + g].astype(jnp.float32)
        pieces.append(jnp.maximum(piece, 0.0).astype(jnp.bfloat16).astype(jnp.float32))
    values = jnp.concatenate(pieces, axis=1)
    gain = jnp.concatenate([gain_ref[n : n + 1, :] for n in range(gain_ref.shape[0])], axis=1)
    inverse_rms = lax.rsqrt(jnp.mean(values * values, axis=1, keepdims=True) + epsilon)
    out_ref[...] = (values * inverse_rms * gain.astype(jnp.float32)).astype(jnp.bfloat16)


def per_device(
    features,
    adjacency,
    source_block,
    edge_type,
    target_block,
    live_count,
    relation_weight,
    self_weight,
    layer_bias,
    norm_gain,
):
    peers = lax.axis_size("dp")
    groups = lax.axis_size("mp")
    rows, width = features.shape
    relations, _, columns = relation_weight.shape
    blocks = rows // BLK
    outer = peers // PAIR
    part = rows // groups
    vmem = pl.BlockSpec(memory_space=pltpu.VMEM)
    hbm = pl.BlockSpec(memory_space=pl.ANY)
    dma = pltpu.SemaphoreType.DMA
    return pl.pallas_call(
        functools.partial(kernel, peers, groups),
        out_shape=jax.ShapeDtypeStruct((part, width), jnp.bfloat16),
        in_specs=[hbm] * 10,
        out_specs=vmem,
        scratch_shapes=[
            pltpu.VMEM(features.shape, jnp.bfloat16),
            pltpu.SMEM(source_block.shape, jnp.int32),
            pltpu.SMEM(edge_type.shape, jnp.int32),
            pltpu.VMEM(target_block.shape, jnp.int32),
            pltpu.SMEM(live_count.shape, jnp.int32),
            pltpu.VMEM(self_weight.shape, jnp.bfloat16),
            pltpu.VMEM((1, columns), jnp.bfloat16),
            pltpu.VMEM((width // LANES, LANES), jnp.bfloat16),
            pltpu.VMEM(adjacency.shape, jnp.bfloat16),
            pltpu.VMEM(relation_weight.shape, jnp.bfloat16),
            pltpu.VMEM((blocks * relations + 1, BLK, columns), jnp.bfloat16),
            pltpu.VMEM((peers, 1, LANES), jnp.int32),
            pltpu.VMEM((peers, 1, LANES), jnp.int32),
            pltpu.SMEM((peers, 1, LANES), jnp.int32),
            pltpu.VMEM((rows, columns), jnp.float32),
            pltpu.VMEM((outer, rows, columns), jnp.bfloat16),
            pltpu.VMEM((outer, rows, columns), jnp.bfloat16),
            pltpu.VMEM((outer, rows, columns), jnp.bfloat16),
            pltpu.VMEM((outer * groups, part, columns), jnp.bfloat16),
            dma((8,)),
            dma((relations // 2,)),
            dma((peers,)),
            dma((peers,)),
            dma((peers,)),
            dma,
            dma((outer,)),
            dma((outer,)),
            dma((outer, groups)),
            dma((outer * groups,)),
        ],
        compiler_params=pltpu.CompilerParams(collective_id=0, has_side_effects=True),
    )(
        features,
        source_block,
        edge_type,
        target_block,
        live_count,
        self_weight,
        layer_bias.reshape(1, columns),
        norm_gain.reshape(width // LANES, LANES),
        adjacency,
        relation_weight,
    )


def solution(mesh):
    return jax.shard_map(
        per_device,
        mesh=mesh,
        in_specs=(
            P("dp", None),
            P("dp", None, None, None),
            P("dp", None),
            P("dp", None),
            P("dp", None),
            P("dp", None),
            P(None, None, "mp"),
            P(None, "mp"),
            P("mp"),
            P(),
        ),
        out_specs=P(("dp", "mp"), None),
        check_vma=False,
    )
```
